512 devices in a mesh: pipe: 16 (over x_lo, y, core), expert: 32 (over z, x_hi).
Axes of the slice: x: 4 (x_hi: 2, x_lo: 2; x = x_hi * 2 + x_lo), y: 4, z: 16, core: 2. Of those that a mesh axis runs over, the one named last changes fastest.
Arguments:
- forward_tokens: bfloat16 [16, 768, 3584], P('pipe', 'expert'), may hold values from -6 to 6
- forward_routing: int32 [16, 768, 1], P('pipe', 'expert'), may hold values from 0 to 3; in each aligned block of 24 rows (0 to 23, 24 to 47, ..., all dimensions but the last counted through in order) at most 8 rows name the same one
- forward_gates: float32 [16, 768], P('pipe', 'expert'), may hold values from 0.25 to 2.5
- backward_tokens: bfloat16 [16, 768, 3584], P('pipe', 'expert'), may hold values from -6 to 6
- backward_routing: int32 [16, 768, 1], P('pipe', 'expert'), may hold values from 0 to 3; in each aligned block of 24 rows (0 to 23, 24 to 47, ..., all dimensions but the last counted through in order) at most 8 rows name the same one
- backward_gates: float32 [16, 768], P('pipe', 'expert'), may hold values from 0.25 to 2.5
- cotangent: bfloat16 [16, 768, 3584], P('pipe', 'expert'), may hold values from -6 to 6
- gate_matrix: bfloat16 [16, 3584, 4096], P('pipe', None, 'expert'), as said below
- up_matrix: bfloat16 [16, 3584, 4096], P('pipe', None, 'expert'), as said below
- down_matrix: bfloat16 [16, 4096, 3584], P('pipe', 'expert'), as said below
Outputs:
- forward_output: bfloat16 [16, 768, 3584], P('pipe', 'expert')
- input_gradient: bfloat16 [16, 768, 3584], P('pipe', 'expert')
- gate_gradient: bfloat16 [16, 1792, 4096], P('pipe', None, 'expert')
- up_gradient: bfloat16 [16, 1792, 4096], P('pipe', None, 'expert')
- down_gradient: bfloat16 [16, 4096, 1792], P('pipe', 'expert')
The draws below stay inside these ranges and needn't reach their ends.
Inputs may be any that keep to these rules, and one draw needn't show every extreme that they name: `forward_routing`: in each device's 24 rows no expert is named more than 8 times. `backward_routing`: in each device's 24 rows no expert is named more than 8 times. `gate_matrix`: blocks p and 15 - p along the first dimension are equal. `up_matrix`: blocks p and 15 - p along the first dimension are equal. `down_matrix`: blocks p and 15 - p along the first dimension are equal.
All inputs are finite; a program needn't handle non-finite values.
Results may differ from the reference program's by a relative error of at most 0.0065.
Values may be sent and summed in bfloat16 or wider, within the bound.
No kernel may reach another device: no remote copies, remote signals or barrier semaphores. Data moves between devices by JAX's collectives and lax.ppermute only.
A program may use at most 64 MiB of HBM per device.

```python
import math
import jax
import jax.numpy as jnp
import numpy as np
from jax import lax

MODEL_WIDTH = 3584
HID = 1024
SHARING_CARDS = 8
TOK = 24
EXPERTS = 4
HIDDEN_PER_CARD = 128
CAP = 8
N_PIPE = 16
N_EXPERT = 32


def mirrored(key, shape_half, factor):
    value_entries = jax.random.truncated_normal(key, -4.0, 4.0, shape_half, jnp.float32) * factor
    return jnp.concatenate([value_entries, value_entries[::-1]], axis=0)


def draw_gate_matrix(key, part):
    return mirrored(jax.random.fold_in(key, 11), (N_PIPE // 2, MODEL_WIDTH, N_EXPERT * HIDDEN_PER_CARD), MODEL_WIDTH ** (-0.5)).astype(jnp.bfloat16)


def draw_up_matrix(key, part):
    return mirrored(jax.random.fold_in(key, 23), (N_PIPE // 2, MODEL_WIDTH, N_EXPERT * HIDDEN_PER_CARD), MODEL_WIDTH ** (-0.5)).astype(jnp.bfloat16)


def draw_down_matrix(key, part):
    return mirrored(jax.random.fold_in(key, 37), (N_PIPE // 2, N_EXPERT * HIDDEN_PER_CARD, MODEL_WIDTH), HID ** (-0.5)).astype(jnp.bfloat16)


def level_of(stream_key, dims, shards, low, high):
    def one(axis_at, parts):
        steps = jax.random.uniform(jax.random.fold_in(jax.random.fold_in(stream_key, 6), axis_at), (parts,), jnp.float32, low / len(shards), high / len(shards))
        return jnp.repeat(jnp.exp(steps), dims[axis_at] // parts).reshape((-1,) + (1,) * (len(dims) - axis_at - 1))

    factor_of = one(*shards[0])
    for cut in shards[1:]:
        factor_of = factor_of * one(*cut)
    return factor_of


def deal_out(key, own, number, rows, number_of, top, bound, skew):
    sequence = jax.random.permutation(key, number_of)
    heavy_load, usual = portions_of(number_of, rows * top, bound, skew, True), portions_of(number_of, rows * top, bound, skew, False)
    places = jnp.arange(number_of)

    def named(tallies, rotation):
        used = int((tallies > 0).sum())
        fixed = max(1, used // 4)
        passed = fixed + (places - fixed + rotation * (used - fixed)) % max(1, number_of - fixed)
        return jnp.zeros((number_of,), jnp.int32).at[sequence[jnp.where(places < fixed, places, passed)]].set(jnp.asarray(tallies, jnp.int32))

    tallies = jnp.where(number % 4 == 0, named(heavy_load, number // 4), named(usual, number - number // 4 - 1))
    mixed = jax.random.permutation(jax.random.fold_in(own, 3), number_of)
    donor, sink = mixed[0:number_of // 2 * 2:2], mixed[1:number_of // 2 * 2:2]
    slack = jnp.minimum(tallies[donor] - 1, bound - tallies[sink]) // 2
    slack = jnp.where((donor == sequence[0]) | (sink == sequence[0]) | (tallies[sink] == 0), 0, jnp.maximum(slack, 0))
    passed = jax.random.randint(jax.random.fold_in(own, 4), (number_of // 2,), 0, 1 << 20) % (slack + 1)
    tallies = tallies.at[donor].add(-passed).at[sink].add(passed)
    labels = jnp.searchsorted(jnp.cumsum(tallies), jnp.arange(rows * top), side="right").astype(jnp.int32)
    listing = labels.reshape(top, rows).T
    listing = listing[jax.random.permutation(jax.random.fold_in(own, 1), rows)]
    rotation = jax.random.randint(jax.random.fold_in(own, 2), (rows, 1), 0, top)
    return jnp.take_along_axis(listing, (jnp.arange(top)[None, :] + rotation) % top, axis=1)


def portions_of(count, total, reach, slope, full):
    weights = [(1 << 20) // math.isqrt(grade ** slope) + 1 for grade in range(1, count + 1)]
    largest = reach if full else min(reach, max(-(-total // count), total * weights[0] // sum(weights)))
    least = 1 if total - largest >= count - 1 else 0
    given, surplus = [largest] + [least] * (count - 1), total - largest - least * (count - 1)
    while surplus > 0:
        free = [i for i in range(1, count) if given[i] < largest] or [i for i in range(1, count) if given[i] < reach]
        mass, budget = sum([weights[i] for i in free]), surplus
        for i in free:
            addition = min(reach - given[i], max(1, budget * weights[i] // mass), surplus)
            given[i] = given[i] + addition
            surplus = surplus - addition
    return np.array(given)


def centred(own_key, extent, width, bound, split=(), held_as=jnp.bfloat16):
    array = width * jax.random.normal(own_key, extent, jnp.float32)
    if split:
        array = array * level_of(own_key, extent, split, -0.22, 0.18)
    return jnp.clip(array, -bound, bound).astype(held_as)


def setup_inputs(seed: int = 0) -> dict:
    keys = jax.random.split(jax.random.key(seed), 11)
    forward_tokens = centred(keys[0], (N_PIPE, N_EXPERT * TOK, MODEL_WIDTH), 1.0, 6.0, ((0, 16), (1, 32)))
    forward_routing_keys = jax.random.split(jax.random.fold_in(keys[1], 1), N_PIPE * (N_EXPERT * TOK) // TOK)
    forward_routing_turns = jax.random.permutation(jax.random.fold_in(keys[1], 3), N_PIPE * (N_EXPERT * TOK) // TOK)
    forward_routing = jax.vmap(lambda own, number: deal_out(jax.random.fold_in(keys[1], 2), own, number, TOK, EXPERTS, 1, CAP, 2))(forward_routing_keys, forward_routing_turns).reshape((N_PIPE, N_EXPERT * TOK, 1))
    forward_gates = jnp.clip(jnp.exp(math.log(2.5) - 2.3025851 * jax.random.uniform(keys[2], (N_PIPE, N_EXPERT * TOK), jnp.float32) ** level_of(keys[2], (N_PIPE, N_EXPERT * TOK), ((0, 16), (1, 32)), -0.2, 0.2)), 0.25, 2.5)
    backward_tokens = centred(keys[3], (N_PIPE, N_EXPERT * TOK, MODEL_WIDTH), 1.0, 6.0, ((0, 16), (1, 32)))
    backward_routing_keys = jax.random.split(jax.random.fold_in(keys[4], 1), N_PIPE * (N_EXPERT * TOK) // TOK)
    backward_routing_turns = jax.random.permutation(jax.random.fold_in(keys[4], 3), N_PIPE * (N_EXPERT * TOK) // TOK)
    backward_routing = jax.vmap(lambda own, number: deal_out(jax.random.fold_in(keys[4], 2), own, number, TOK, EXPERTS, 1, CAP, 2))(backward_routing_keys, backward_routing_turns).reshape((N_PIPE, N_EXPERT * TOK, 1))
    backward_gates = jnp.clip(jnp.exp(math.log(2.5) - 2.3025851 * jax.random.uniform(keys[5], (N_PIPE, N_EXPERT * TOK), jnp.float32) ** level_of(keys[5], (N_PIPE, N_EXPERT * TOK), ((0, 16), (1, 32)), -0.2, 0.2)), 0.25, 2.5)
    cotangent = centred(keys[6], (N_PIPE, N_EXPERT * TOK, MODEL_WIDTH), 1.0, 6.0, ((0, 16), (1, 32)))
    gate_matrix = draw_gate_matrix(jax.random.fold_in(keys[10], 71), 0)
    up_matrix = draw_up_matrix(jax.random.fold_in(keys[10], 71), 0)
    down_matrix = draw_down_matrix(jax.random.fold_in(keys[10], 71), 0)
    return {"forward_tokens": forward_tokens, "forward_routing": forward_routing, "forward_gates": forward_gates, "backward_tokens": backward_tokens, "backward_routing": backward_routing, "backward_gates": backward_gates, "cotangent": cotangent, "gate_matrix": gate_matrix, "up_matrix": up_matrix, "down_matrix": down_matrix}


def row_places(routing):
    sources = routing.reshape(N_EXPERT, TOK)
    members = (sources[:, :, None] == jnp.arange(EXPERTS, dtype=jnp.int32)[None, None, :]).astype(jnp.int32)
    earlier = jnp.cumsum(members, axis=1) - members
    within = jnp.sum(earlier * members, axis=2)
    anchors = jnp.arange(N_EXPERT, dtype=jnp.int32)[:, None]
    return (sources * (N_EXPERT * CAP) + anchors * CAP + within).reshape(-1).astype(jnp.int32)


def expert_rows(value_entries, places):
    zeroed = jnp.zeros((EXPERTS * N_EXPERT * CAP, MODEL_WIDTH), value_entries.dtype)
    return zeroed.at[places].set(value_entries).reshape(EXPERTS, N_EXPERT * CAP, MODEL_WIDTH)


def member_parts(left_section, right_section):
    return jnp.einsum("wey,eyk->wek", left_section.reshape(-1, SHARING_CARDS, HIDDEN_PER_CARD).astype(jnp.float32), right_section.reshape(SHARING_CARDS, HIDDEN_PER_CARD, MODEL_WIDTH).astype(jnp.float32))


def rounded_total(partials):
    rounded = lax.optimization_barrier(partials.astype(jnp.bfloat16))
    return jnp.sum(rounded.astype(jnp.float32), axis=1)


def expert_forward(item):
    rows, gate_block, up_block, down_block = item
    gate_pre = jnp.dot(rows, gate_block, preferred_element_type=jnp.float32)
    up_pre = jnp.dot(rows, up_block, preferred_element_type=jnp.float32)
    hidden = (jax.nn.silu(gate_pre) * up_pre).astype(jnp.bfloat16)
    return rounded_total(member_parts(hidden, down_block))


def expert_backward(item):
    rows, grads, gate_block, up_block, down_block = item
    gate_pre = jnp.dot(rows, gate_block, preferred_element_type=jnp.float32)
    up_pre = jnp.dot(rows, up_block, preferred_element_type=jnp.float32)
    sigma = jax.nn.sigmoid(gate_pre)
    activated = gate_pre * sigma
    hidden = (activated * up_pre).astype(jnp.bfloat16)
    hidden_grad = jnp.dot(grads, down_block.T, preferred_element_type=jnp.float32)
    gate_grad = (hidden_grad * up_pre * sigma * (1.0 + gate_pre * (1.0 - sigma))).astype(jnp.bfloat16)
    up_grad = (hidden_grad * activated).astype(jnp.bfloat16)
    summed = rounded_total(member_parts(gate_grad, gate_block.T) + member_parts(up_grad, up_block.T))
    gate_weight_grad = jnp.dot(rows.T, gate_grad, preferred_element_type=jnp.float32).astype(jnp.bfloat16)
    up_weight_grad = jnp.dot(rows.T, up_grad, preferred_element_type=jnp.float32).astype(jnp.bfloat16)
    down_weight_grad = jnp.dot(hidden.T, grads, preferred_element_type=jnp.float32).astype(jnp.bfloat16)
    return summed, gate_weight_grad, up_weight_grad, down_weight_grad


def position(forward_tokens, forward_routing, forward_gates, backward_tokens, backward_routing, backward_gates, cotangent, gate_matrix, up_matrix, down_matrix):
    gate_blocks = gate_matrix.reshape(MODEL_WIDTH, EXPERTS, HID).transpose(1, 0, 2)
    up_blocks = up_matrix.reshape(MODEL_WIDTH, EXPERTS, HID).transpose(1, 0, 2)
    down_blocks = down_matrix.reshape(EXPERTS, HID, MODEL_WIDTH)
    forward_places = row_places(forward_routing)
    forward_row_set = expert_rows(forward_tokens, forward_places)
    forward_sums = lax.map(expert_forward, (forward_row_set, gate_blocks, up_blocks, down_blocks)).reshape(-1, MODEL_WIDTH)
    forward_result = (forward_gates[:, None] * forward_sums[forward_places]).astype(jnp.bfloat16)
    scaled = (backward_gates[:, None] * cotangent.astype(jnp.float32)).astype(jnp.bfloat16)
    backward_places = row_places(backward_routing)
    backward_rows = expert_rows(backward_tokens, backward_places)
    scaled_rows = expert_rows(scaled, backward_places)
    backward_sums, gate_grads, up_grads, down_grads = lax.map(expert_backward, (backward_rows, scaled_rows, gate_blocks, up_blocks, down_blocks))
    backward_result = backward_sums.reshape(-1, MODEL_WIDTH)[backward_places].astype(jnp.bfloat16)
    gate_total = gate_grads.transpose(1, 0, 2).reshape(MODEL_WIDTH, EXPERTS * HID)
    up_total = up_grads.transpose(1, 0, 2).reshape(MODEL_WIDTH, EXPERTS * HID)
    down_total = down_grads.reshape(EXPERTS * HID, MODEL_WIDTH)
    return forward_result, backward_result, gate_total, up_total, down_total


def reference(forward_tokens, forward_routing, forward_gates, backward_tokens, backward_routing, backward_gates, cotangent, gate_matrix, up_matrix, down_matrix):
    middle = MODEL_WIDTH // 2

    def at_position(where):
        return position(forward_tokens[where], forward_routing[where, :, 0], forward_gates[where], backward_tokens[where], backward_routing[where, :, 0], backward_gates[where], cotangent[where], gate_matrix[where], up_matrix[where], down_matrix[where])

    def mirrored_pair(lower):
        upper = N_PIPE - 1 - lower
        first = at_position(lower)
        second = at_position(upper)
        first_grads = lax.optimization_barrier(first[2:])
        second_grads = lax.optimization_barrier(second[2:])
        totals = [(left_grad.astype(jnp.float32) + right_grad.astype(jnp.float32)).astype(jnp.bfloat16) for left_grad, right_grad in zip(first_grads, second_grads)]
        return (first[0], first[1], second[0], second[1], totals[0][:middle], totals[0][middle:], totals[1][:middle], totals[1][middle:], totals[2][:, :middle], totals[2][:, middle:])

    results = lax.map(mirrored_pair, jnp.arange(N_PIPE // 2, dtype=jnp.int32))

    def joined(lower_blocks, upper_blocks):
        return jnp.concatenate([lower_blocks, upper_blocks[::-1]], axis=0)

    return (joined(results[0], results[2]), joined(results[1], results[3]), joined(results[4], results[5]), joined(results[6], results[7]), joined(results[8], results[9]))
```

```python
import jax
import jax.numpy as jnp
from jax import lax
from jax.sharding import PartitionSpec as P

SHARING_CARDS = 8
CONTRACT_LAST = (((1,), (1,)), ((), ()))
CONTRACT_FIRST = (((0,), (0,)), ((), ()))


def swap(value, axis, mask):
    pairs = [(source, source ^ mask) for source in range(lax.axis_size(axis))]
    return lax.ppermute(value, axis, pairs)


def mirror(value):
    positions = lax.axis_size("pipe")
    pairs = [(source, positions - 1 - source) for source in range(positions)]
    return lax.ppermute(value, "pipe", pairs)


def after(value, *others):
    return lax.optimization_barrier((value, *others))[0]


def dot(left, right, dims=(((1,), (0,)), ((), ()))):
    return lax.dot_general(left, right, dims, preferred_element_type=jnp.float32)


def slot_matrix(labels, experts, capacity):
    members = (labels[:, None] == jnp.arange(experts, dtype=jnp.int32)[None, :]).astype(jnp.int32)
    earlier = jnp.cumsum(members, axis=0) - members
    within = jnp.sum(earlier * members, axis=1)
    target = labels * capacity + within
    matches = target[None, :] == jnp.arange(experts * capacity, dtype=jnp.int32)[:, None]
    return matches.astype(jnp.bfloat16)


def on_device(
    forward_tokens,
    forward_routing,
    forward_gates,
    backward_tokens,
    backward_routing,
    backward_gates,
    cotangent,
    gate_matrix,
    up_matrix,
    down_matrix,
):
    devices = lax.axis_size("expert")
    experts = devices // SHARING_CARDS
    lines = SHARING_CARDS // 2
    tokens = forward_tokens.shape[1]
    width = forward_tokens.shape[2]
    capacity = max(tokens // 3, tokens // experts)
    own_group = lax.axis_index("expert") // SHARING_CARDS
    line_groups = [
        [SHARING_CARDS * a + 2 * j + h for j in range(lines)] for a in range(experts) for h in range(2)
    ]
    gate_weights = gate_matrix[0]
    up_weights = up_matrix[0]
    down_weights = down_matrix[0]
    scaled = (backward_gates[0][:, None] * cotangent[0].astype(jnp.float32)).astype(jnp.bfloat16)
    forward_slots = slot_matrix(forward_routing[0, :, 0] ^ own_group, experts, capacity)
    backward_slots = slot_matrix(backward_routing[0, :, 0] ^ own_group, experts, capacity)

    tall = experts * capacity
    placed = [
        dot(slots, rows).astype(jnp.bfloat16)
        for slots, rows in (
            (backward_slots, backward_tokens[0]),
            (backward_slots, scaled),
            (forward_slots, forward_tokens[0]),
        )
    ]
    blocks = jnp.stack([block.reshape(experts, capacity, width) for block in placed], axis=1)
    arrived = [blocks[0]] + [swap(blocks[k], "expert", SHARING_CARDS * k) for k in range(1, experts)]

    def line_gather(value):
        return lax.all_gather(value, "expert", axis_index_groups=line_groups, tiled=True)

    held = [jnp.concatenate([block[i] for block in arrived], axis=0) for i in range(3)]
    rows_own = line_gather(held[0])
    rows_other = swap(rows_own, "expert", 1)
    grads_own = line_gather(after(held[1], rows_own))
    grads_other = swap(grads_own, "expert", 1)
    ahead_own = line_gather(after(held[2], grads_own))
    ahead_other = swap(ahead_own, "expert", 1)

    def line_sum(kept, received):
        total = (kept + received.astype(jnp.float32)).astype(jnp.bfloat16)
        parts = lax.all_to_all(
            total.reshape(lines, tall, width),
            "expert",
            split_axis=0,
            concat_axis=0,
            axis_index_groups=line_groups,
            tiled=True,
        )
        return parts.astype(jnp.float32).sum(axis=0).astype(jnp.bfloat16)

    def give_back(summed, slots):
        stacked = summed.reshape(experts, capacity, width)
        back = [stacked[0]] + [
            swap(stacked[k], "expert", SHARING_CARDS * k) for k in range(1, experts)
        ]
        return dot(slots, jnp.concatenate(back, axis=0), CONTRACT_FIRST)

    def backward_half(rows, grads):
        gate_pre = dot(rows, gate_weights)
        up_pre = dot(rows, up_weights)
        sigma = jax.nn.sigmoid(gate_pre)
        activated = gate_pre * sigma
        hidden = (activated * up_pre).astype(jnp.bfloat16)
        hidden_grad = dot(grads, down_weights, CONTRACT_LAST)
        gate_grad = (hidden_grad * up_pre * sigma * (1.0 + gate_pre * (1.0 - sigma))).astype(
            jnp.bfloat16
        )
        up_grad = (hidden_grad * activated).astype(jnp.bfloat16)
        return hidden, gate_grad, up_grad

    def backward_parts(gate_grad, up_grad):
        return dot(gate_grad, gate_weights, CONTRACT_LAST) + dot(
            up_grad, up_weights, CONTRACT_LAST
        )

    def forward_parts(rows):
        gate_pre = dot(rows, gate_weights)
        up_pre = dot(rows, up_weights)
        hidden = (jax.nn.silu(gate_pre) * up_pre).astype(jnp.bfloat16)
        return dot(hidden, down_weights)

    other = backward_half(rows_other, grads_other)
    backward_sent = swap(backward_parts(*other[1:]).astype(jnp.bfloat16), "expert", 1)
    own = backward_half(rows_own, grads_own)
    backward_kept = backward_parts(*own[1:])

    middle = width // 2
    upper_side = (lax.axis_index("pipe") >= lax.axis_size("pipe") // 2).astype(jnp.int32)

    def partial_of(start):
        def columns(value):
            return lax.dynamic_slice_in_dim(value, start, middle, 1)

        y_own, y_other = columns(rows_own), columns(rows_other)
        g_own, g_other = columns(grads_own), columns(grads_other)
        gate = dot(y_own, own[1], CONTRACT_FIRST) + dot(y_other, other[1], CONTRACT_FIRST)
        up = dot(y_own, own[2], CONTRACT_FIRST) + dot(y_other, other[2], CONTRACT_FIRST)
        down = dot(own[0], g_own, CONTRACT_FIRST) + dot(other[0], g_other, CONTRACT_FIRST)
        return [value.astype(jnp.bfloat16) for value in (gate, up, down)]

    outgoing = [mirror(value) for value in partial_of((1 - upper_side) * middle)]
    retained = partial_of(upper_side * middle)

    forward_sent = swap(forward_parts(ahead_other).astype(jnp.bfloat16), "expert", 1)
    forward_kept = forward_parts(ahead_own)

    backward_total = line_sum(backward_kept, backward_sent)
    backward_result = give_back(backward_total, backward_slots).astype(jnp.bfloat16)
    forward_total = line_sum(forward_kept, forward_sent)
    forward_result = (
        forward_gates[0][:, None] * give_back(forward_total, forward_slots)
    ).astype(jnp.bfloat16)

    gradients = [
        (kept.astype(jnp.float32) + came.astype(jnp.float32)).astype(jnp.bfloat16)[None]
        for kept, came in zip(retained, outgoing)
    ]
    return forward_result[None], backward_result[None], *gradients


def solution(mesh):
    in_specs = (
        P("pipe", "expert", None),
        P("pipe", "expert", None),
        P("pipe", "expert"),
        P("pipe", "expert", None),
        P("pipe", "expert", None),
        P("pipe", "expert"),
        P("pipe", "expert", None),
        P("pipe", None, "expert"),
        P("pipe", None, "expert"),
        P("pipe", "expert", None),
    )
    out_specs = (
        P("pipe", "expert", None),
        P("pipe", "expert", None),
        P("pipe", None, "expert"),
        P("pipe", None, "expert"),
        P("pipe", "expert", None),
    )
    return jax.shard_map(
        on_device, mesh=mesh, in_specs=in_specs, out_specs=out_specs, check_vma=False
    )
```

```python
import jax
import jax.numpy as jnp
from jax import lax
from jax.sharding import PartitionSpec as P

SHARING_CARDS = 8
CONTRACT_LAST = (((1,), (1,)), ((), ()))
CONTRACT_FIRST = (((0,), (0,)), ((), ()))


def swap(value, axis, mask):
    pairs = [(source, source ^ mask) for source in range(lax.axis_size(axis))]
    return lax.ppermute(value, axis, pairs)


def mirror(value):
    positions = lax.axis_size("pipe")
    pairs = [(source, positions - 1 - source) for source in range(positions)]
    return lax.ppermute(value, "pipe", pairs)


def after(value, *others):
    return lax.optimization_barrier((value, *others))[0]


def dot(left, right, dims=(((1,), (0,)), ((), ()))):
    return lax.dot_general(left, right, dims, preferred_element_type=jnp.float32)


def slot_matrix(labels, experts, capacity):
    members = (labels[:, None] == jnp.arange(experts, dtype=jnp.int32)[None, :]).astype(jnp.int32)
    earlier = jnp.cumsum(members, axis=0) - members
    within = jnp.sum(earlier * members, axis=1)
    target = labels * capacity + within
    matches = target[None, :] == jnp.arange(experts * capacity, dtype=jnp.int32)[:, None]
    return matches.astype(jnp.bfloat16)


def on_device(
    forward_tokens,
    forward_routing,
    forward_gates,
    backward_tokens,
    backward_routing,
    backward_gates,
    cotangent,
    gate_matrix,
    up_matrix,
    down_matrix,
):
    devices = lax.axis_size("expert")
    experts = devices // SHARING_CARDS
    lines = SHARING_CARDS // 2
    tokens = forward_tokens.shape[1]
    width = forward_tokens.shape[2]
    capacity = max(tokens // 3, tokens // experts)
    own_group = lax.axis_index("expert") // SHARING_CARDS
    line_groups = [
        [SHARING_CARDS * a + 2 * j + h for j in range(lines)] for a in range(experts) for h in range(2)
    ]
    gate_weights = gate_matrix[0]
    up_weights = up_matrix[0]
    down_weights = down_matrix[0]
    partner_gate, partner_up, partner_down = [
        swap(value, "expert", 1) for value in (gate_weights, up_weights, down_weights)
    ]
    scaled = (backward_gates[0][:, None] * cotangent[0].astype(jnp.float32)).astype(jnp.bfloat16)
    order = sorted(range(experts), key=lambda step: (step != 0, step != 2, step))

    def slots_of(routing):
        step = routing[0, :, 0] ^ own_group
        place = sum((step == order[j]) * j for j in range(1, experts)).astype(jnp.int32)
        return slot_matrix(place, experts, capacity)

    forward_slots = slots_of(forward_routing)
    backward_slots = slots_of(backward_routing)

    tall = experts * capacity

    def send_out(*row_sets):
        blocks = jnp.stack(
            [
                dot(slots, rows).astype(jnp.bfloat16).reshape(experts, capacity, width)
                for slots, rows in row_sets
            ],
            axis=1,
        )
        arrived = [
            swap(blocks[j], "expert", SHARING_CARDS * order[j]) if j else blocks[j]
            for j in range(experts)
        ]
        arrived[1:] = after(arrived[1:], partner_gate, partner_up)
        return [
            jnp.concatenate([block[i] for block in arrived], axis=0) for i in range(len(row_sets))
        ]

    def line_gather(value):
        return lax.all_gather(value, "expert", axis_index_groups=line_groups, tiled=True)

    rows_held, grads_held, ahead_held = send_out(
        (backward_slots, backward_tokens[0]), (backward_slots, scaled), (forward_slots, forward_tokens[0])
    )
    rows_own = line_gather(rows_held)
    rows_other = swap(rows_own, "expert", 1)
    grads_own = line_gather(after(grads_held, rows_own, partner_down))
    grads_other = swap(after(grads_own, rows_other), "expert", 1)
    ahead = line_gather(after(ahead_held, grads_own, rows_other))
    ahead = after(ahead, grads_other)

    def line_sum(values):
        parts = lax.all_to_all(
            values,
            "expert",
            split_axis=0,
            concat_axis=0,
            axis_index_groups=line_groups,
            tiled=True,
        )
        return parts.astype(jnp.float32).sum(axis=0)

    def give_back(*summed):
        blocks = jnp.stack(
            [value.astype(jnp.bfloat16).reshape(experts, capacity, width) for value in summed], axis=1
        )
        return [
            swap(blocks[j], "expert", SHARING_CARDS * order[j]) if j else blocks[j]
            for j in range(experts)
        ]

    def joined(back, i):
        return jnp.concatenate([block[i] for block in back], axis=0)

    def backward_half(rows, grads):
        gate_pre = dot(rows, gate_weights)
        up_pre = dot(rows, up_weights)
        sigma = jax.nn.sigmoid(gate_pre)
        activated = gate_pre * sigma
        hidden = (activated * up_pre).astype(jnp.bfloat16)
        hidden_grad = dot(grads, down_weights, CONTRACT_LAST)
        gate_grad = (hidden_grad * up_pre * sigma * (1.0 + gate_pre * (1.0 - sigma))).astype(
            jnp.bfloat16
        )
        up_grad = (hidden_grad * activated).astype(jnp.bfloat16)
        return hidden, gate_grad, up_grad

    def backward_parts(gate_grad, up_grad):
        return dot(gate_grad, gate_weights, CONTRACT_LAST) + dot(
            up_grad, up_weights, CONTRACT_LAST
        )

    def forward_slice(gate_slice, up_slice, down_slice):
        gate_pre = dot(ahead, gate_slice)
        up_pre = dot(ahead, up_slice)
        hidden = (jax.nn.silu(gate_pre) * up_pre).astype(jnp.bfloat16)
        return dot(hidden, down_slice)

    forward_parts = forward_slice(gate_weights, up_weights, down_weights) + forward_slice(
        partner_gate, partner_up, partner_down
    )
    forward_total = line_sum(forward_parts.astype(jnp.bfloat16).reshape(lines, tall, width))

    grads_other = after(grads_other, forward_parts)
    other = backward_half(rows_other, grads_other)
    backward_leaving = backward_parts(*other[1:]).astype(jnp.bfloat16)
    backward_sent = swap(backward_leaving, "expert", 1)

    own = backward_half(rows_own, grads_own)
    backward_kept = backward_parts(*own[1:])
    backward_sent = after(backward_sent, forward_total)
    backward_pair = (backward_kept + backward_sent.astype(jnp.float32)).astype(jnp.bfloat16)
    backward_total = line_sum(backward_pair.reshape(lines, tall, width))

    middle = width // 2
    upper_side = (lax.axis_index("pipe") >= lax.axis_size("pipe") // 2).astype(jnp.int32)

    def partial_of(start):
        def columns(value):
            return lax.dynamic_slice_in_dim(value, start, middle, 1)

        y_own, y_other = columns(rows_own), columns(rows_other)
        g_own, g_other = columns(grads_own), columns(grads_other)
        gate = dot(y_own, own[1], CONTRACT_FIRST) + dot(y_other, other[1], CONTRACT_FIRST)
        up = dot(y_own, own[2], CONTRACT_FIRST) + dot(y_other, other[2], CONTRACT_FIRST)
        down = dot(g_own, own[0], CONTRACT_FIRST) + dot(g_other, other[0], CONTRACT_FIRST)
        return jnp.stack([value.astype(jnp.bfloat16) for value in (gate, up, down)])

    outgoing = mirror(after(partial_of((1 - upper_side) * middle), backward_pair))
    retained = partial_of(upper_side * middle)

    back = give_back(forward_total, backward_total)
    forward_back, backward_back = joined(back, 0), joined(back, 1)
    forward_result = (
        forward_gates[0][:, None] * dot(forward_slots, forward_back, CONTRACT_FIRST)
    ).astype(jnp.bfloat16)
    backward_result = dot(backward_slots, backward_back, CONTRACT_FIRST).astype(jnp.bfloat16)

    outgoing = after(outgoing, back[1])
    gradients = (retained.astype(jnp.float32) + outgoing.astype(jnp.float32)).astype(jnp.bfloat16)
    return (
        forward_result[None],
        backward_result[None],
        gradients[0][None],
        gradients[1][None],
        gradients[2].T[None],
    )


def solution(mesh):
    in_specs = (
        P("pipe", "expert", None),
        P("pipe", "expert", None),
        P("pipe", "expert"),
        P("pipe", "expert", None),
        P("pipe", "expert", None),
        P("pipe", "expert"),
        P("pipe", "expert", None),
        P("pipe", None, "expert"),
        P("pipe", None, "expert"),
        P("pipe", "expert", None),
    )
    out_specs = (
        P("pipe", "expert", None),
        P("pipe", "expert", None),
        P("pipe", None, "expert"),
        P("pipe", None, "expert"),
        P("pipe", "expert", None),
    )
    return jax.shard_map(
        on_device, mesh=mesh, in_specs=in_specs, out_specs=out_specs, check_vma=False
    )
```

```python
import jax
import jax.numpy as jnp
from jax import lax
from jax.experimental import pallas as pl
from jax.experimental.pallas import tpu as pltpu
from jax.sharding import PartitionSpec as P

SHARING_CARDS = 8
CONTRACT_LAST = (((1,), (1,)), ((), ()))
CONTRACT_FIRST = (((0,), (0,)), ((), ()))


def swap(value, axis, mask):
    pairs = [(source, source ^ mask) for source in range(lax.axis_size(axis))]
    return lax.ppermute(value, axis, pairs)


def mirror(value):
    positions = lax.axis_size("pipe")
    pairs = [(source, positions - 1 - source) for source in range(positions)]
    return lax.ppermute(value, "pipe", pairs)


def after(value, *others):
    return lax.optimization_barrier((value, *others))[0]


def dot(left, right, dims=(((1,), (0,)), ((), ()))):
    return lax.dot_general(left, right, dims, preferred_element_type=jnp.float32)


def slot_matrix(labels, experts, capacity):
    members = (labels[:, None] == jnp.arange(experts, dtype=jnp.int32)[None, :]).astype(jnp.int32)
    earlier = jnp.cumsum(members, axis=0) - members
    within = jnp.sum(earlier * members, axis=1)
    target = labels * capacity + within
    matches = target[None, :] == jnp.arange(experts * capacity, dtype=jnp.int32)[:, None]
    return matches.astype(jnp.bfloat16)


def forward_kernel(x_ref, gate_a, up_a, down_a, gate_b, up_b, down_b, out_ref):
    x = x_ref[...]
    hidden = []
    for gate_ref, up_ref in ((gate_a, up_a), (gate_b, up_b)):
        gate_pre = jnp.dot(x, gate_ref[...], preferred_element_type=jnp.float32)
        up_pre = jnp.dot(x, up_ref[...], preferred_element_type=jnp.float32)
        hidden.append((gate_pre / (1.0 + jnp.exp(-gate_pre)) * up_pre).astype(jnp.bfloat16))
    step = 512
    for start in range(0, out_ref.shape[1], step):
        cut = slice(start, start + step)
        total = jnp.dot(hidden[0], down_a[:, cut], preferred_element_type=jnp.float32)
        total += jnp.dot(hidden[1], down_b[:, cut], preferred_element_type=jnp.float32)
        out_ref[:, cut] = total.astype(jnp.bfloat16)


def forward_block(x, own, partner):
    rows, width = x.shape
    units = own[0].shape[1]
    return pl.pallas_call(
        forward_kernel,
        out_shape=jax.ShapeDtypeStruct(x.shape, jnp.bfloat16),
        in_specs=[pl.BlockSpec(memory_space=pltpu.VMEM)] * 7,
        out_specs=pl.BlockSpec(memory_space=pltpu.VMEM),
        cost_estimate=pl.CostEstimate(
            flops=12 * rows * width * units,
            bytes_accessed=2 * (2 * rows * width + 6 * width * units),
            transcendentals=2 * rows * units,
        ),
        compiler_params=pltpu.CompilerParams(vmem_limit_bytes=24 * 2**20),
    )(x, *own, *partner)


def backward_kernel(x_ref, g_ref, gate_ref, up_ref, down_ref, parts_ref, gate_grad_ref, up_grad_ref, hidden_ref):
    x = x_ref[...]
    gate_pre = jnp.dot(x, gate_ref[...], preferred_element_type=jnp.float32)
    up_pre = jnp.dot(x, up_ref[...], preferred_element_type=jnp.float32)
    hidden_grad = dot(g_ref[...], down_ref[...], CONTRACT_LAST)
    sigma = 1.0 / (1.0 + jnp.exp(-gate_pre))
    activated = gate_pre * sigma
    hidden_ref[...] = (activated * up_pre).astype(jnp.bfloat16)
    gate_grad = (hidden_grad * up_pre * sigma * (1.0 + gate_pre * (1.0 - sigma))).astype(jnp.bfloat16)
    up_grad = (hidden_grad * activated).astype(jnp.bfloat16)
    gate_grad_ref[...] = gate_grad
    up_grad_ref[...] = up_grad
    step = 512
    for start in range(0, x_ref.shape[1], step):
        cut = slice(start, start + step)
        total = dot(gate_grad, gate_ref[cut, :], CONTRACT_LAST)
        total += dot(up_grad, up_ref[cut, :], CONTRACT_LAST)
        parts_ref[:, cut] = total.astype(parts_ref.dtype)


def backward_block(x, g, gate, up, down, parts_type):
    rows, width = x.shape
    units = gate.shape[1]
    small = jax.ShapeDtypeStruct((rows, units), jnp.bfloat16)
    return pl.pallas_call(
        backward_kernel,
        out_shape=[jax.ShapeDtypeStruct(x.shape, parts_type), small, small, small],
        in_specs=[pl.BlockSpec(memory_space=pltpu.VMEM)] * 5,
        out_specs=[pl.BlockSpec(memory_space=pltpu.VMEM)] * 4,
        cost_estimate=pl.CostEstimate(
            flops=10 * rows * width * units,
            bytes_accessed=2 * (4 * rows * width + 3 * width * units),
            transcendentals=rows * units,
        ),
        compiler_params=pltpu.CompilerParams(vmem_limit_bytes=24 * 2**20),
    )(x, g, gate, up, down)


def on_device(
    forward_tokens,
    forward_routing,
    forward_gates,
    backward_tokens,
    backward_routing,
    backward_gates,
    cotangent,
    gate_matrix,
    up_matrix,
    down_matrix,
):
    devices = lax.axis_size("expert")
    experts = devices // SHARING_CARDS
    lines = SHARING_CARDS // 2
    tokens = forward_tokens.shape[1]
    width = forward_tokens.shape[2]
    capacity = max(tokens // 3, tokens // experts)
    own_group = lax.axis_index("expert") // SHARING_CARDS
    line_groups = [
        [SHARING_CARDS * a + 2 * j + h for j in range(lines)] for a in range(experts) for h in range(2)
    ]
    gate_weights = gate_matrix[0]
    up_weights = up_matrix[0]
    down_weights = down_matrix[0]
    partner_gate, partner_up, partner_down = [
        swap(value, "expert", 1) for value in (gate_weights, up_weights, down_weights)
    ]
    scaled = (backward_gates[0][:, None] * cotangent[0].astype(jnp.float32)).astype(jnp.bfloat16)
    order = sorted(range(experts), key=lambda step: (step != 0, step != 2, step))

    def slots_of(routing):
        step = routing[0, :, 0] ^ own_group
        place = sum((step == order[j]) * j for j in range(1, experts)).astype(jnp.int32)
        return slot_matrix(place, experts, capacity)

    forward_slots = slots_of(forward_routing)
    backward_slots = slots_of(backward_routing)

    tall = experts * capacity

    def send_out(*row_sets):
        blocks = jnp.stack(
            [
                dot(slots, rows).astype(jnp.bfloat16).reshape(experts, capacity, width)
                for slots, rows in row_sets
            ],
            axis=1,
        )
        arrived = [
            swap(blocks[j], "expert", SHARING_CARDS * order[j]) if j else blocks[j]
            for j in range(experts)
        ]
        arrived[1:] = after(arrived[1:], partner_gate)
        return [
            jnp.concatenate([block[i] for block in arrived], axis=0) for i in range(len(row_sets))
        ]

    def line_gather(value):
        return lax.all_gather(value, "expert", axis_index_groups=line_groups, tiled=True)

    rows_held, grads_held, ahead_held = send_out(
        (backward_slots, backward_tokens[0]), (backward_slots, scaled), (forward_slots, forward_tokens[0])
    )
    rows_own = line_gather(rows_held)
    rows_other = swap(rows_own, "expert", 1)
    grads_own = line_gather(after(grads_held, rows_own, partner_up, partner_down))
    grads_other = swap(after(grads_own, rows_other), "expert", 1)
    ahead = line_gather(after(ahead_held, grads_own, rows_other))
    ahead = after(ahead, grads_other)

    def line_sum(values):
        parts = lax.all_to_all(
            values,
            "expert",
            split_axis=0,
            concat_axis=0,
            axis_index_groups=line_groups,
            tiled=True,
        )
        return parts.astype(jnp.float32).sum(axis=0)

    def give_back(*summed):
        blocks = jnp.stack(
            [value.astype(jnp.bfloat16).reshape(experts, capacity, width) for value in summed], axis=1
        )
        return [
            swap(blocks[j], "expert", SHARING_CARDS * order[j]) if j else blocks[j]
            for j in range(experts)
        ]

    def joined(back, i):
        return jnp.concatenate([block[i] for block in back], axis=0)

    forward_parts = forward_block(
        ahead, (gate_weights, up_weights, down_weights), (partner_gate, partner_up, partner_down)
    )
    forward_total = line_sum(forward_parts.reshape(lines, tall, width))
    grads_other = after(grads_other, forward_parts)
    weights = (gate_weights, up_weights, down_weights)
    backward_leaving, *other = backward_block(rows_other, grads_other, *weights, jnp.bfloat16)
    backward_sent = swap(backward_leaving, "expert", 1)

    backward_kept, *own = backward_block(rows_own, grads_own, *weights, jnp.float32)
    backward_sent = after(backward_sent, forward_total)
    backward_pair = (backward_kept + backward_sent.astype(jnp.float32)).astype(jnp.bfloat16)
    backward_total = line_sum(backward_pair.reshape(lines, tall, width))

    middle = width // 2
    upper_side = (lax.axis_index("pipe") >= lax.axis_size("pipe") // 2).astype(jnp.int32)

    def partial_of(start):
        def columns(value):
            return lax.dynamic_slice_in_dim(value, start, middle, 1)

        y_own, y_other = columns(rows_own), columns(rows_other)
        g_own, g_other = columns(grads_own), columns(grads_other)
        gate = dot(y_own, own[0], CONTRACT_FIRST) + dot(y_other, other[0], CONTRACT_FIRST)
        up = dot(y_own, own[1], CONTRACT_FIRST) + dot(y_other, other[1], CONTRACT_FIRST)
        down = dot(g_own, own[2], CONTRACT_FIRST) + dot(g_other, other[2], CONTRACT_FIRST)
        return [value.astype(jnp.bfloat16) for value in (gate, up, down)]

    leaving = jnp.stack(partial_of((1 - upper_side) * middle))
    outgoing = mirror(after(leaving, backward_pair))
    retained = partial_of(upper_side * middle)

    back = give_back(forward_total, backward_total)
    forward_back, backward_back = joined(back, 0), joined(back, 1)
    outgoing = after(outgoing, back[1])
    gate_result, up_result, down_result = [
        (kept.astype(jnp.float32) + outgoing[i].astype(jnp.float32)).astype(jnp.bfloat16)
        for i, kept in enumerate(retained)
    ]
    forward_back, backward_back = after([forward_back, backward_back], gate_result, up_result, down_result)
    forward_result = (
        forward_gates[0][:, None] * dot(forward_slots, forward_back, CONTRACT_FIRST)
    ).astype(jnp.bfloat16)
    backward_result = dot(backward_slots, backward_back, CONTRACT_FIRST).astype(jnp.bfloat16)

    return (
        forward_result[None],
        backward_result[None],
        gate_result[None],
        up_result[None],
        down_result.T[None],
    )


def solution(mesh):
    in_specs = (
        P("pipe", "expert", None),
        P("pipe", "expert", None),
        P("pipe", "expert"),
        P("pipe", "expert", None),
        P("pipe", "expert", None),
        P("pipe", "expert"),
        P("pipe", "expert", None),
        P("pipe", None, "expert"),
        P("pipe", None, "expert"),
        P("pipe", "expert", None),
    )
    out_specs = (
        P("pipe", "expert", None),
        P("pipe", "expert", None),
        P("pipe", None, "expert"),
        P("pipe", None, "expert"),
        P("pipe", "expert", None),
    )
    return jax.shard_map(
        on_device, mesh=mesh, in_specs=in_specs, out_specs=out_specs, check_vma=False
    )
```

```python
import jax
import jax.numpy as jnp
from jax import lax
from jax.experimental import pallas as pl
from jax.experimental.pallas import tpu as pltpu
from jax.sharding import PartitionSpec as P

SHARING_CARDS = 8
CONTRACT_LAST = (((1,), (1,)), ((), ()))
CONTRACT_FIRST = (((0,), (0,)), ((), ()))


def swap(value, axis, mask):
    pairs = [(source, source ^ mask) for source in range(lax.axis_size(axis))]
    return lax.ppermute(value, axis, pairs)


def mirror(value):
    positions = lax.axis_size("pipe")
    pairs = [(source, positions - 1 - source) for source in range(positions)]
    return lax.ppermute(value, "pipe", pairs)


def after(value, *others):
    return lax.optimization_barrier((value, *others))[0]


def dot(left, right, dims=(((1,), (0,)), ((), ()))):
    return lax.dot_general(left, right, dims, preferred_element_type=jnp.float32)


def slot_matrix(labels, experts, capacity):
    members = (labels[:, None] == jnp.arange(experts, dtype=jnp.int32)[None, :]).astype(jnp.int32)
    earlier = jnp.cumsum(members, axis=0) - members
    within = jnp.sum(earlier * members, axis=1)
    target = labels * capacity + within
    matches = target[None, :] == jnp.arange(experts * capacity, dtype=jnp.int32)[:, None]
    return matches.astype(jnp.bfloat16)


def forward_kernel(x_ref, gate_a, up_a, down_a, gate_b, up_b, down_b, out_ref):
    x = x_ref[...]
    hidden = []
    for gate_ref, up_ref in ((gate_a, up_a), (gate_b, up_b)):
        gate_pre = jnp.dot(x, gate_ref[...], preferred_element_type=jnp.float32)
        up_pre = jnp.dot(x, up_ref[...], preferred_element_type=jnp.float32)
        hidden.append((gate_pre / (1.0 + jnp.exp(-gate_pre)) * up_pre).astype(jnp.bfloat16))
    step = 512
    for start in range(0, out_ref.shape[1], step):
        cut = slice(start, start + step)
        total = jnp.dot(hidden[0], down_a[:, cut], preferred_element_type=jnp.float32)
        total += jnp.dot(hidden[1], down_b[:, cut], preferred_element_type=jnp.float32)
        out_ref[:, cut] = total.astype(jnp.bfloat16)


def forward_block(x, own, partner):
    rows, width = x.shape
    units = own[0].shape[1]
    return pl.pallas_call(
        forward_kernel,
        out_shape=jax.ShapeDtypeStruct(x.shape, jnp.bfloat16),
        in_specs=[pl.BlockSpec(memory_space=pltpu.VMEM)] * 7,
        out_specs=pl.BlockSpec(memory_space=pltpu.VMEM),
        cost_estimate=pl.CostEstimate(
            flops=12 * rows * width * units,
            bytes_accessed=2 * (2 * rows * width + 6 * width * units),
            transcendentals=2 * rows * units,
        ),
        compiler_params=pltpu.CompilerParams(vmem_limit_bytes=24 * 2**20),
    )(x, *own, *partner)


def on_device(
    forward_tokens,
    forward_routing,
    forward_gates,
    backward_tokens,
    backward_routing,
    backward_gates,
    cotangent,
    gate_matrix,
    up_matrix,
    down_matrix,
):
    devices = lax.axis_size("expert")
    experts = devices // SHARING_CARDS
    lines = SHARING_CARDS // 2
    tokens = forward_tokens.shape[1]
    width = forward_tokens.shape[2]
    capacity = max(tokens // 3, tokens // experts)
    own_group = lax.axis_index("expert") // SHARING_CARDS
    line_groups = [
        [SHARING_CARDS * a + 2 * j + h for j in range(lines)] for a in range(experts) for h in range(2)
    ]
    gate_weights = gate_matrix[0]
    up_weights = up_matrix[0]
    down_weights = down_matrix[0]
    partner_gate, partner_up, partner_down = [
        swap(value, "expert", 1) for value in (gate_weights, up_weights, down_weights)
    ]
    scaled = (backward_gates[0][:, None] * cotangent[0].astype(jnp.float32)).astype(jnp.bfloat16)
    order = sorted(range(experts), key=lambda step: (step != 0, step != 2, step))

    def slots_of(routing):
        step = routing[0, :, 0] ^ own_group
        place = sum((step == order[j]) * j for j in range(1, experts)).astype(jnp.int32)
        return slot_matrix(place, experts, capacity)

    forward_slots = slots_of(forward_routing)
    backward_slots = slots_of(backward_routing)

    tall = experts * capacity

    def send_out(*row_sets):
        blocks = jnp.stack(
            [
                dot(slots, rows).astype(jnp.bfloat16).reshape(experts, capacity, width)
                for slots, rows in row_sets
            ],
            axis=1,
        )
        arrived = [
            swap(blocks[j], "expert", SHARING_CARDS * order[j]) if j else blocks[j]
            for j in range(experts)
        ]
        arrived[1:] = after(arrived[1:], partner_gate)
        return [
            jnp.concatenate([block[i] for block in arrived], axis=0) for i in range(len(row_sets))
        ]

    def line_gather(value):
        return lax.all_gather(value, "expert", axis_index_groups=line_groups, tiled=True)

    rows_held, grads_held, ahead_held = send_out(
        (backward_slots, backward_tokens[0]), (backward_slots, scaled), (forward_slots, forward_tokens[0])
    )
    rows_own = line_gather(rows_held)
    rows_other = swap(rows_own, "expert", 1)
    grads_own = line_gather(after(grads_held, rows_own, partner_up, partner_down))
    grads_other = swap(after(grads_own, rows_other), "expert", 1)
    ahead = line_gather(after(ahead_held, grads_own, rows_other))
    ahead = after(ahead, grads_other)

    def line_sum(values):
        parts = lax.all_to_all(
            values,
            "expert",
            split_axis=0,
            concat_axis=0,
            axis_index_groups=line_groups,
            tiled=True,
        )
        return parts.astype(jnp.float32).sum(axis=0)

    def give_back(*summed):
        blocks = jnp.stack(
            [value.astype(jnp.bfloat16).reshape(experts, capacity, width) for value in summed], axis=1
        )
        return [
            swap(blocks[j], "expert", SHARING_CARDS * order[j]) if j else blocks[j]
            for j in range(experts)
        ]

    def joined(back, i):
        return jnp.concatenate([block[i] for block in back], axis=0)

    def backward_half(rows, grads):
        gate_pre = dot(rows, gate_weights)
        up_pre = dot(rows, up_weights)
        sigma = jax.nn.sigmoid(gate_pre)
        activated = gate_pre * sigma
        hidden = (activated * up_pre).astype(jnp.bfloat16)
        hidden_grad = dot(grads, down_weights, CONTRACT_LAST)
        gate_grad = (hidden_grad * up_pre * sigma * (1.0 + gate_pre * (1.0 - sigma))).astype(
            jnp.bfloat16
        )
        up_grad = (hidden_grad * activated).astype(jnp.bfloat16)
        return hidden, gate_grad, up_grad

    def backward_parts(gate_grad, up_grad):
        return dot(gate_grad, gate_weights, CONTRACT_LAST) + dot(
            up_grad, up_weights, CONTRACT_LAST
        )

    forward_parts = forward_block(
        ahead, (gate_weights, up_weights, down_weights), (partner_gate, partner_up, partner_down)
    )
    forward_total = line_sum(forward_parts.reshape(lines, tall, width))
    grads_other = after(grads_other, forward_parts)
    other = backward_half(rows_other, grads_other)
    backward_leaving = backward_parts(*other[1:]).astype(jnp.bfloat16)
    backward_sent = swap(backward_leaving, "expert", 1)

    own = backward_half(rows_own, grads_own)
    backward_kept = backward_parts(*own[1:])
    backward_sent = after(backward_sent, forward_total)
    backward_pair = (backward_kept + backward_sent.astype(jnp.float32)).astype(jnp.bfloat16)
    backward_total = line_sum(backward_pair.reshape(lines, tall, width))

    middle = width // 2
    upper_side = (lax.axis_index("pipe") >= lax.axis_size("pipe") // 2).astype(jnp.int32)

    def partial_of(start):
        def columns(value):
            return lax.dynamic_slice_in_dim(value, start, middle, 1)

        y_own, y_other = columns(rows_own), columns(rows_other)
        g_own, g_other = columns(grads_own), columns(grads_other)
        gate = dot(y_own, own[1], CONTRACT_FIRST) + dot(y_other, other[1], CONTRACT_FIRST)
        up = dot(y_own, own[2], CONTRACT_FIRST) + dot(y_other, other[2], CONTRACT_FIRST)
        down = dot(g_own, own[0], CONTRACT_FIRST) + dot(g_other, other[0], CONTRACT_FIRST)
        return jnp.stack([value.astype(jnp.bfloat16) for value in (gate, up, down)])

    outgoing = mirror(after(partial_of((1 - upper_side) * middle), backward_pair))
    retained = partial_of(upper_side * middle)

    back = give_back(forward_total, backward_total)
    forward_back, backward_back = joined(back, 0), joined(back, 1)
    forward_result = (
        forward_gates[0][:, None] * dot(forward_slots, forward_back, CONTRACT_FIRST)
    ).astype(jnp.bfloat16)
    backward_result = dot(backward_slots, backward_back, CONTRACT_FIRST).astype(jnp.bfloat16)

    outgoing = after(outgoing, back[1])
    gradients = (retained.astype(jnp.float32) + outgoing.astype(jnp.float32)).astype(jnp.bfloat16)
    return (
        forward_result[None],
        backward_result[None],
        gradients[0][None],
        gradients[1][None],
        gradients[2].T[None],
    )


def solution(mesh):
    in_specs = (
        P("pipe", "expert", None),
        P("pipe", "expert", None),
        P("pipe", "expert"),
        P("pipe", "expert", None),
        P("pipe", "expert", None),
        P("pipe", "expert"),
        P("pipe", "expert", None),
        P("pipe", None, "expert"),
        P("pipe", None, "expert"),
        P("pipe", "expert", None),
    )
    out_specs = (
        P("pipe", "expert", None),
        P("pipe", "expert", None),
        P("pipe", None, "expert"),
        P("pipe", None, "expert"),
        P("pipe", "expert", None),
    )
    return jax.shard_map(
        on_device, mesh=mesh, in_specs=in_specs, out_specs=out_specs, check_vma=False
    )
```

```python
import jax
import jax.numpy as jnp
from jax import lax
from jax.experimental import pallas as pl
from jax.experimental.pallas import tpu as pltpu
from jax.sharding import PartitionSpec as P

SHARING_CARDS = 8
CONTRACT_LAST = (((1,), (1,)), ((), ()))
CONTRACT_FIRST = (((0,), (0,)), ((), ()))


def swap(value, axis, mask):
    pairs = [(source, source ^ mask) for source in range(lax.axis_size(axis))]
    return lax.ppermute(value, axis, pairs)


def mirror(value):
    positions = lax.axis_size("pipe")
    pairs = [(source, positions - 1 - source) for source in range(positions)]
    return lax.ppermute(value, "pipe", pairs)


def after(value, *others):
    return lax.optimization_barrier((value, *others))[0]


def dot(left, right, dims=(((1,), (0,)), ((), ()))):
    return lax.dot_general(left, right, dims, preferred_element_type=jnp.float32)


def slot_matrix(labels, experts, capacity):
    members = (labels[:, None] == jnp.arange(experts, dtype=jnp.int32)[None, :]).astype(jnp.int32)
    earlier = jnp.cumsum(members, axis=0) - members
    within = jnp.sum(earlier * members, axis=1)
    target = labels * capacity + within
    matches = target[None, :] == jnp.arange(experts * capacity, dtype=jnp.int32)[:, None]
    return matches.astype(jnp.bfloat16)


def forward_kernel(x_ref, gate_a, up_a, down_a, gate_b, up_b, down_b, out_ref):
    x = x_ref[...]
    hidden = []
    for gate_ref, up_ref in ((gate_a, up_a), (gate_b, up_b)):
        gate_pre = jnp.dot(x, gate_ref[...], preferred_element_type=jnp.float32)
        up_pre = jnp.dot(x, up_ref[...], preferred_element_type=jnp.float32)
        hidden.append((gate_pre / (1.0 + jnp.exp(-gate_pre)) * up_pre).astype(jnp.bfloat16))
    step = 512
    for start in range(0, out_ref.shape[1], step):
        cut = slice(start, start + step)
        total = jnp.dot(hidden[0], down_a[:, cut], preferred_element_type=jnp.float32)
        total += jnp.dot(hidden[1], down_b[:, cut], preferred_element_type=jnp.float32)
        out_ref[:, cut] = total.astype(jnp.bfloat16)


def forward_block(x, own, partner):
    rows, width = x.shape
    units = own[0].shape[1]
    return pl.pallas_call(
        forward_kernel,
        out_shape=jax.ShapeDtypeStruct(x.shape, jnp.bfloat16),
        in_specs=[pl.BlockSpec(memory_space=pltpu.VMEM)] * 7,
        out_specs=pl.BlockSpec(memory_space=pltpu.VMEM),
        cost_estimate=pl.CostEstimate(
            flops=12 * rows * width * units,
            bytes_accessed=2 * (2 * rows * width + 6 * width * units),
            transcendentals=2 * rows * units,
        ),
        compiler_params=pltpu.CompilerParams(vmem_limit_bytes=24 * 2**20),
    )(x, *own, *partner)


def on_device(
    forward_tokens,
    forward_routing,
    forward_gates,
    backward_tokens,
    backward_routing,
    backward_gates,
    cotangent,
    gate_matrix,
    up_matrix,
    down_matrix,
):
    devices = lax.axis_size("expert")
    experts = devices // SHARING_CARDS
    lines = SHARING_CARDS // 2
    tokens = forward_tokens.shape[1]
    width = forward_tokens.shape[2]
    capacity = max(tokens // 3, tokens // experts)
    own_group = lax.axis_index("expert") // SHARING_CARDS
    line_groups = [
        [SHARING_CARDS * a + 2 * j + h for j in range(lines)] for a in range(experts) for h in range(2)
    ]
    gate_weights = gate_matrix[0]
    up_weights = up_matrix[0]
    down_weights = down_matrix[0]
    partner_gate, partner_up, partner_down = [
        swap(value, "expert", 1) for value in (gate_weights, up_weights, down_weights)
    ]
    scaled = (backward_gates[0][:, None] * cotangent[0].astype(jnp.float32)).astype(jnp.bfloat16)
    order = sorted(range(experts), key=lambda step: (step != 0, step != 2, step))

    def slots_of(routing):
        step = routing[0, :, 0] ^ own_group
        place = sum((step == order[j]) * j for j in range(1, experts)).astype(jnp.int32)
        return slot_matrix(place, experts, capacity)

    forward_slots = slots_of(forward_routing)
    backward_slots = slots_of(backward_routing)

    tall = experts * capacity

    def send_out(*row_sets):
        blocks = jnp.stack(
            [
                dot(slots, rows).astype(jnp.bfloat16).reshape(experts, capacity, width)
                for slots, rows in row_sets
            ],
            axis=1,
        )
        arrived = [
            swap(blocks[j], "expert", SHARING_CARDS * order[j]) if j else blocks[j]
            for j in range(experts)
        ]
        arrived[1:] = after(arrived[1:], partner_gate)
        return [
            jnp.concatenate([block[i] for block in arrived], axis=0) for i in range(len(row_sets))
        ]

    def line_gather(value):
        return lax.all_gather(value, "expert", axis_index_groups=line_groups, tiled=True)

    rows_held, grads_held, ahead_held = send_out(
        (backward_slots, backward_tokens[0]), (backward_slots, scaled), (forward_slots, forward_tokens[0])
    )
    rows_own = line_gather(rows_held)
    rows_other = swap(rows_own, "expert", 1)
    grads_own = line_gather(after(grads_held, rows_own, partner_up, partner_down))
    grads_other = swap(after(grads_own, rows_other), "expert", 1)
    ahead = line_gather(after(ahead_held, grads_own, rows_other))
    ahead = after(ahead, grads_other)

    def line_sum(values):
        parts = lax.all_to_all(
            values,
            "expert",
            split_axis=0,
            concat_axis=0,
            axis_index_groups=line_groups,
            tiled=True,
        )
        return parts.astype(jnp.float32).sum(axis=0)

    def give_back(*summed):
        blocks = jnp.stack(
            [value.astype(jnp.bfloat16).reshape(experts, capacity, width) for value in summed], axis=1
        )
        return [
            swap(blocks[j], "expert", SHARING_CARDS * order[j]) if j else blocks[j]
            for j in range(experts)
        ]

    def joined(back, i):
        return jnp.concatenate([block[i] for block in back], axis=0)

    def backward_half(rows, grads):
        gate_pre = dot(rows, gate_weights)
        up_pre = dot(rows, up_weights)
        sigma = jax.nn.sigmoid(gate_pre)
        activated = gate_pre * sigma
        hidden = (activated * up_pre).astype(jnp.bfloat16)
        hidden_grad = dot(grads, down_weights, CONTRACT_LAST)
        gate_grad = (hidden_grad * up_pre * sigma * (1.0 + gate_pre * (1.0 - sigma))).astype(
            jnp.bfloat16
        )
        up_grad = (hidden_grad * activated).astype(jnp.bfloat16)
        return hidden, gate_grad, up_grad

    def backward_parts(gate_grad, up_grad):
        return dot(gate_grad, gate_weights, CONTRACT_LAST) + dot(
            up_grad, up_weights, CONTRACT_LAST
        )

    forward_parts = forward_block(
        ahead, (gate_weights, up_weights, down_weights), (partner_gate, partner_up, partner_down)
    )
    forward_total = line_sum(forward_parts.reshape(lines, tall, width))
    grads_other = after(grads_other, forward_parts)
    other = backward_half(rows_other, grads_other)
    backward_leaving = backward_parts(*other[1:]).astype(jnp.bfloat16)
    backward_sent = swap(backward_leaving, "expert", 1)

    own = backward_half(rows_own, grads_own)
    backward_kept = backward_parts(*own[1:])
    backward_sent = after(backward_sent, forward_total)
    backward_pair = (backward_kept + backward_sent.astype(jnp.float32)).astype(jnp.bfloat16)
    backward_total = line_sum(backward_pair.reshape(lines, tall, width))

    middle = width // 2
    upper_side = (lax.axis_index("pipe") >= lax.axis_size("pipe") // 2).astype(jnp.int32)

    def partial_of(start):
        def columns(value):
            return lax.dynamic_slice_in_dim(value, start, middle, 1)

        y_own, y_other = columns(rows_own), columns(rows_other)
        g_own, g_other = columns(grads_own), columns(grads_other)
        gate = dot(y_own, own[1], CONTRACT_FIRST) + dot(y_other, other[1], CONTRACT_FIRST)
        up = dot(y_own, own[2], CONTRACT_FIRST) + dot(y_other, other[2], CONTRACT_FIRST)
        down = dot(g_own, own[0], CONTRACT_FIRST) + dot(g_other, other[0], CONTRACT_FIRST)
        return jnp.stack([value.astype(jnp.bfloat16) for value in (gate, up, down)])

    outgoing = mirror(after(partial_of((1 - upper_side) * middle), backward_pair))
    retained = partial_of(upper_side * middle)

    back = give_back(forward_total, backward_total)
    forward_back, backward_back = joined(back, 0), joined(back, 1)
    outgoing = after(outgoing, back[1])
    gradients = (retained.astype(jnp.float32) + outgoing.astype(jnp.float32)).astype(jnp.bfloat16)
    down_result = gradients[2].T
    backward_back = after(backward_back, down_result)
    forward_result = (
        forward_gates[0][:, None] * dot(forward_slots, forward_back, CONTRACT_FIRST)
    ).astype(jnp.bfloat16)
    backward_result = dot(backward_slots, backward_back, CONTRACT_FIRST).astype(jnp.bfloat16)

    return (
        forward_result[None],
        backward_result[None],
        gradients[0][None],
        gradients[1][None],
        down_result[None],
    )


def solution(mesh):
    in_specs = (
        P("pipe", "expert", None),
        P("pipe", "expert", None),
        P("pipe", "expert"),
        P("pipe", "expert", None),
        P("pipe", "expert", None),
        P("pipe", "expert"),
        P("pipe", "expert", None),
        P("pipe", None, "expert"),
        P("pipe", None, "expert"),
        P("pipe", "expert", None),
    )
    out_specs = (
        P("pipe", "expert", None),
        P("pipe", "expert", None),
        P("pipe", None, "expert"),
        P("pipe", None, "expert"),
        P("pipe", "expert", None),
    )
    return jax.shard_map(
        on_device, mesh=mesh, in_specs=in_specs, out_specs=out_specs, check_vma=False
    )
```
